128 devices in a mesh: tm: 16 (over y, x), row: 8 (over z, core).
Axes of the slice: x: 4, y: 4, z: 4, core: 2. Of those that a mesh axis runs over, the one named last changes fastest.
Arguments:
- starts: float32 [16, 8, 16384], P('tm', None, 'row'), may hold values from -6 to 6
- operator: float32 [16384, 16384], P('row', 'tm'), may hold values from -1 to 1
- coarse_left: float32 [16384, 256], P('row'), may hold values from -0.375 to 0.375
- coarse_right: float32 [16384, 256], P('row'), may hold values from -0.046875 to 0.046875
Outputs:
- new_ends: float32 [16, 8, 16384], P('tm', None, 'row')
The draws below stay inside these ranges and needn't reach their ends.
All inputs are finite; a program needn't handle non-finite values.
Results may differ from the reference program's by a relative error of at most 0.00019.
Values sent between devices are 32-bit elements; how exact they have to be, the bound alone decides.
A program may use at most 64 MiB of HBM per device.

```python
import jax
import jax.numpy as jnp
from jax import lax

N = 16384
R = 256
E = 8
FINE = 4
SLICES = 16


def shard_levels(stream_key, dims, pieces, smallest, largest):
    level, own = 1.0, jax.random.fold_in(stream_key, 6)
    for dim, shards_of in pieces:
        draws = jnp.exp(jax.random.uniform(jax.random.fold_in(own, dim), (shards_of,), jnp.float32, smallest / len(pieces), largest / len(pieces)))
        level = level * jnp.repeat(draws, dims[dim] // shards_of).reshape([-1 if axis == dim else 1 for axis in range(len(dims))])
    return level


def bell_draw(key, extent, deviation, most, split=(), dtype=jnp.bfloat16):
    values = jax.random.normal(key, extent, jnp.float32) * deviation
    if len(split) > 0:
        values = shard_levels(key, extent, split, -0.22, 0.18) * values
    return jnp.clip(values, min=-most, max=most).astype(dtype)


def setup_inputs(seed: int = 0) -> dict:
    keys = jax.random.split(jax.random.key(seed), 5)
    starts = bell_draw(keys[0], (SLICES, E, N), 1.0, 6.0, ((0, 16), (2, 8)), jnp.float32)
    operator = bell_draw(keys[1], (N, N), (max(1, 8 * N // (SLICES * FINE) ** 2)) ** -0.5, 1.0, ((0, 8), (1, 16)), jnp.float32)
    coarse_left = bell_draw(keys[2], (N, R), R ** -0.5, 0.375, ((0, 8),), jnp.float32)
    coarse_right = bell_draw(keys[3], (N, R), N ** -0.5, 0.046875, ((0, 8),), jnp.float32)
    return {"starts": starts, "operator": operator, "coarse_left": coarse_left, "coarse_right": coarse_right}


highest = lax.Precision.HIGHEST


def reference(starts, operator, coarse_left, coarse_right):
    slices = starts.shape[0]
    step_time = 1.0 / slices
    fine_time = step_time / FINE
    flattened = starts.reshape(slices * E, N)

    def fine_step(current, unused):
        images = lax.dot_general(current, operator, (((1,), (1,)), ((), ())), precision=highest, preferred_element_type=jnp.float32)
        return current + fine_time * images, None

    flattened, unused_out = lax.scan(fine_step, flattened, None, length=FINE)
    fine_ends = flattened.reshape(slices, E, N)
    old_projection = jnp.einsum("sen,nr->ser", starts, coarse_right, precision=highest)
    defects = fine_ends - (starts + step_time * jnp.einsum("ser,nr->sen", old_projection, coarse_left, precision=highest))

    def sweep_step(current, defect):
        projection = jnp.dot(current, coarse_right, precision=highest, preferred_element_type=jnp.float32)
        following = current + step_time * jnp.dot(projection, coarse_left.T, precision=highest, preferred_element_type=jnp.float32) + defect
        return following, following

    unused_last, new_ends = lax.scan(sweep_step, starts[0], defects)
    return new_ends
```

```python
import functools

import jax
import jax.numpy as jnp
from jax import lax
from jax.experimental import pallas as pl
from jax.experimental.pallas import tpu as pltpu
from jax.sharding import PartitionSpec as P

MESH = pl.DeviceIdType.MESH
F32 = jnp.float32
BF16 = jnp.bfloat16
HIGHEST = lax.Precision.HIGHEST

FINE = 4
SLICES = 16
E = 8
LANES = SLICES * E
STEP_TIME = 1.0 / SLICES
FINE_TIME = STEP_TIME / FINE
BLK = 256


def split(values):
    high = values.astype(BF16)
    low = (values - high.astype(F32)).astype(BF16)
    return high, low


def dot(left, right):
    return jnp.dot(left, right, preferred_element_type=F32)


def exact(left, right):
    return jnp.dot(left, right, precision=HIGHEST, preferred_element_type=F32)


def kernel(
    starts_hbm, a_hbm, l_hbm, r_hbm, out_ref,
    starts_v, next_v, a_st, a_hi, a_lo, l_v, r_v, r_hi, r_lo, lt_hi, lt_lo,
    p0, xb, xx, qb, p1, sb, p2, qf, fx, fs, fy,
    gpart, grs, gown, gmat, kpow, hpart, hrow, hown, hall, scan,
    load_sem, next_sem, p0_ss, p0_rs, p1_ss, p1_rs, p2_ss, p2_rs, x_ss, xp_ss, x_rs,
    fx_ss, fx_rs, fy_ss, fy_rs, g1_ss, g1_rs, g2_ss, g2_rs, h1_ss, h1_rs, h2_ss, h2_rs,
):
    tm = lax.axis_index("tm")
    row = lax.axis_index("row")
    x, y = tm % 4, tm // 4
    z, c = row // 2, row % 2
    home = (x // 2) == c
    diagonal = y == z

    def at(xx_, yy_, zz_, cc_):
        return (yy_ * 4 + xx_, zz_ * 2 + cc_)

    def rcopy(src, dst, ss, rs, device):
        return pltpu.make_async_remote_copy(
            src_ref=src, dst_ref=dst, send_sem=ss, recv_sem=rs, device_id=device, device_id_type=MESH
        )

    me = (tm, row)

    def arrived(dst, ss, rs):
        rcopy(dst, dst, ss, rs, me).wait_recv()

    chunks = a_st.shape[0]
    rows_a = a_st.shape[1]

    def load_a(i):
        return pltpu.make_async_copy(a_hbm.at[pl.ds(i * rows_a, rows_a), :], a_st.at[i], load_sem.at[3 + i])

    load_starts = pltpu.make_async_copy(starts_hbm.at[0], starts_v, load_sem.at[0])
    load_l = pltpu.make_async_copy(l_hbm, l_v, load_sem.at[1])
    load_r = pltpu.make_async_copy(r_hbm, r_v, load_sem.at[2])
    load_starts.start()
    for i in range(chunks):
        load_a(i).start()
    load_l.start()
    load_r.start()

    barrier = pltpu.get_barrier_semaphore()

    def hello(device):
        pl.semaphore_signal(barrier, inc=1, device_id=device, device_id_type=MESH)

    for d in range(1, 16):
        hello(((tm + d) % 16, row))
    for d in range(1, 8):
        hello((tm, (row + d) % 8))

    @pl.when(home)
    def _():
        for t in range(16):
            other = (t, y * 2 + c)

            @pl.when(jnp.logical_not((tm == t) & diagonal))
            def _():
                hello(other)

    own_target = (home & diagonal).astype(jnp.int32)
    pl.semaphore_wait(barrier, 15 + 7 + 8 - own_target)

    load_starts.wait()

    def p0_copy(i):
        h, zz = i // 4, i % 4
        return rcopy(
            starts_v.at[:, pl.ds(pl.multiple_of(i * BLK, BLK), BLK)], p0.at[tm], p0_ss.at[i], p0_rs.at[tm],
            at(2 * c + h, z, zz, c),
        )

    def p0_self(i):
        return home & diagonal & (i // 4 == x % 2) & (i % 4 == z)

    for i in range(8):
        @pl.when(jnp.logical_not(p0_self(i)))
        def _():
            p0_copy(i).start()

        @pl.when(p0_self(i))
        def _():
            p0[tm] = starts_v[:, i * BLK : (i + 1) * BLK]

    next_copy = rcopy(starts_v, next_v, next_sem.at[0], next_sem.at[1], ((tm + 15) % 16, row))

    @pl.when(tm > 0)
    def _():
        next_copy.start()

    for i in range(chunks):
        load_a(i).wait()
        high, low = split(a_st[i])
        a_hi[i * rows_a : (i + 1) * rows_a, :] = high
        a_lo[i * rows_a : (i + 1) * rows_a, :] = low

    def x_send(s, d):
        zz = (z + d) % 4
        return rcopy(xb.at[s, z], xb.at[s, z], x_ss.at[s, d], x_rs.at[s, z], at(x, y, zz, c))

    def partner_send(s, zz):
        return rcopy(xb.at[s, zz], xb.at[s, zz], xp_ss.at[s, zz], x_rs.at[s, zz], at(x, y, z, 1 - c))

    def own_block_ready(s):
        for d in range(1, 4):
            x_send(s, d).start()
        partner_send(s, z).start()

    @pl.when(home)
    def _():
        for t in range(16):
            @pl.when(jnp.logical_not((tm == t) & diagonal))
            def _():
                arrived(p0.at[t], p0_ss.at[0], p0_rs.at[t])
        xb[0, z] = p0[...].reshape(LANES, BLK).T
        own_block_ready(0)

    load_l.wait()
    load_r.wait()
    high, low = split(r_v[...])
    r_hi[...] = high
    r_lo[...] = low
    high, low = split(l_v[...].T)
    lt_hi[...] = high
    lt_lo[...] = low
    gpart[...] = (
        dot(lt_hi[...], r_hi[...]) + dot(lt_hi[...], r_lo[...]) + dot(lt_lo[...], r_hi[...])
    ).reshape(gpart.shape)

    def g1_send(d):
        rr = (row + d) % 8
        return rcopy(gpart.at[rr], grs.at[row], g1_ss.at[d], g1_rs.at[row], (tm, rr))

    def g2_send(d):
        rr = (row + d) % 8
        return rcopy(gown, gmat.at[row], g2_ss.at[d], g2_rs.at[row], (tm, rr))

    for d in range(1, 8):
        g1_send(d).start()

    def x_ready(s):
        @pl.when(home)
        def _():
            for d in range(1, 4):
                zz = (z + d) % 4
                arrived(xb.at[s, zz], x_ss.at[s, d], x_rs.at[s, zz])
                partner_send(s, zz).start()

        @pl.when(jnp.logical_not(home))
        def _():
            for zz in range(4):
                arrived(xb.at[s, zz], x_ss.at[s, 0], x_rs.at[s, zz])

        for zz in range(4):
            high, low = split(xb[s, zz] * FINE_TIME)
            xx[zz * BLK : (zz + 1) * BLK, :LANES] = high
            xx[zz * BLK : (zz + 1) * BLK, LANES:] = low

    def product(i):
        span = pl.ds(pl.multiple_of(i * BLK, BLK), BLK)
        both = dot(a_hi[span, :], xx[...]) + dot(a_lo[span, :], xx[...])
        return both[:, :LANES] + both[:, LANES:]

    def p1_local(i):
        return (2 * c + i // 4) == x

    def p1_send(s, i):
        h, zz = i // 4, i % 4
        return rcopy(qb.at[s, i], p1.at[s, x, zz], p1_ss.at[s, i], p1_rs.at[s, x, zz], at(2 * c + h, y, z, c))

    def p2_local(zz):
        return diagonal & (zz == z)

    def p2_send(s, zz):
        return rcopy(sb.at[s, zz], p2.at[s, y], p2_ss.at[s, zz], p2_rs.at[s, y], at(x, z, zz, c))

    def fine_step(s, carry):
        x_ready(s)

        def block(i, carry):
            value = product(i)

            @pl.when(p1_local(i))
            def _():
                p1[s, x, i % 4] = value

            @pl.when(jnp.logical_not(p1_local(i)))
            def _():
                qb[s, i] = value
                p1_send(s, i).start()

            return carry

        lax.fori_loop(0, 8, block, 0)

        @pl.when(home)
        def _():
            def summed(zz, carry):
                for d in range(1, 4):
                    xs = (x + d) % 4
                    arrived(p1.at[s, xs, zz], p1_ss.at[s, 0], p1_rs.at[s, xs, zz])
                total = (p1[s, 0, zz] + p1[s, 1, zz]) + (p1[s, 2, zz] + p1[s, 3, zz])
                total = total + jnp.where(diagonal, xb[s, zz], 0.0)

                @pl.when(p2_local(zz))
                def _():
                    p2[s, y] = total

                @pl.when(jnp.logical_not(p2_local(zz)))
                def _():
                    sb[s, zz] = total
                    p2_send(s, zz).start()

                return carry

            lax.fori_loop(0, 4, summed, 0)

            for yy in range(4):
                @pl.when(jnp.logical_not(diagonal & (y == yy)))
                def _():
                    arrived(p2.at[s, yy], p2_ss.at[s, 0], p2_rs.at[s, yy])
            xb[s + 1, z] = (p2[s, 0] + p2[s, 1]) + (p2[s, 2] + p2[s, 3])
            own_block_ready(s + 1)

        return carry

    lax.fori_loop(0, FINE - 1, fine_step, 0)

    for d in range(1, 8):
        rr = (row + d) % 8
        arrived(grs.at[rr], g1_ss.at[d], g1_rs.at[rr])
    total = gpart[row]
    for d in range(1, 8):
        total = total + grs[(row + d) % 8]
    gown[...] = total
    gmat[row] = total
    for d in range(1, 8):
        g2_send(d).start()
    for d in range(1, 8):
        rr = (row + d) % 8
        arrived(gmat.at[rr], g2_ss.at[d], g2_rs.at[rr])
    rank = gmat.shape[2]
    unit = (
        lax.broadcasted_iota(jnp.int32, (rank, rank), 0) == lax.broadcasted_iota(jnp.int32, (rank, rank), 1)
    ).astype(F32)
    kpow[0] = unit + STEP_TIME * gmat[...].reshape(rank, rank)
    for i in range(3):
        kpow[i + 1] = exact(kpow[i], kpow[i])

    last = FINE - 1
    x_ready(last)
    later = [((tm <= n) & (tm > 0)).astype(F32) for n in range(SLICES)]
    own_block = (diagonal & home).astype(F32)

    def last_block(i, carry):
        value = product(i)
        mine = own_block * ((i // 4) == (x % 2)).astype(F32)
        value = value + mine * xb[last, i % 4]
        turned = value.T.reshape(SLICES, E, BLK)
        span = pl.ds(pl.multiple_of(i * BLK, BLK), BLK)
        base = starts_v[:, span]
        running = turned[0]
        qf[0, 0, :, span] = running - later[0] * base
        for n in range(1, SLICES):
            running = running + turned[n]
            qf[n // 4, n % 4, :, span] = running - later[n] * base
        return carry

    lax.fori_loop(0, 8, last_block, 0)

    def fx_send(d):
        xs = (x + d) % 4
        return rcopy(qf.at[:, xs], fx.at[x], fx_ss.at[d], fx_rs.at[x], at(xs, y, z, c))

    def fy_send(d):
        ys = (y + d) % 4
        return rcopy(fs.at[ys], fy.at[y], fy_ss.at[d], fy_rs.at[y], at(x, ys, z, c))

    for d in range(1, 4):
        fx_send(d).start()
    for d in range(1, 4):
        xs = (x + d) % 4
        arrived(fx.at[xs], fx_ss.at[d], fx_rs.at[xs])
    for d in range(4):
        ys = (y + d) % 4
        fs[ys] = (qf[ys, x] + fx[(x + 1) % 4, ys]) + (fx[(x + 2) % 4, ys] + fx[(x + 3) % 4, ys])
    for d in range(1, 4):
        fy_send(d).start()
    for d in range(1, 4):
        ys = (y + d) % 4
        arrived(fy.at[ys], fy_ss.at[d], fy_rs.at[ys])
    total = (fs[y] + fy[(y + 1) % 4]) + (fy[(y + 2) % 4] + fy[(y + 3) % 4])
    fy[y] = total

    @pl.when(tm < 15)
    def _():
        arrived(next_v, next_sem.at[0], next_sem.at[1])

    @pl.when(tm == 15)
    def _():
        next_v[...] = jnp.zeros_like(next_v)

    high, low = split(total - next_v[...])
    hpart[...] = dot(high, r_hi[...]) + dot(high, r_lo[...]) + dot(low, r_hi[...])

    def h1_send(d):
        rr = (row + d) % 8
        return rcopy(hpart, hrow.at[row], h1_ss.at[d], h1_rs.at[row], (tm, rr))

    def h2_send(d):
        tt = (tm + d) % 16
        return rcopy(hown, hall.at[tm + 1], h2_ss.at[d], h2_rs.at[tm], (tt, row))

    for d in range(1, 8):
        h1_send(d).start()
    for d in range(1, 8):
        rr = (row + d) % 8
        arrived(hrow.at[rr], h1_ss.at[d], h1_rs.at[rr])
    hrow[row] = hpart[...]
    total = hrow[0]
    for i in range(1, 8):
        total = total + hrow[i]
    hown[...] = total
    hall[tm + 1] = total
    hall[0] = jnp.zeros_like(total)
    for d in range(1, 16):
        h2_send(d).start()
    for d in range(1, 16):
        tt = (tm + d) % 16
        arrived(hall.at[tt + 1], h2_ss.at[d], h2_rs.at[tt])
    values = hall[0:SLICES].reshape(LANES, rank)
    for i in range(4):
        shift = E << i
        moved = jnp.concatenate([jnp.zeros((shift, rank), F32), values[: LANES - shift]], axis=0)
        values = values + exact(moved, kpow[i])
    scan[...] = values.reshape(scan.shape)
    high, low = split(scan[tm] * STEP_TIME)
    spread = dot(high, lt_hi[...]) + dot(high, lt_lo[...]) + dot(low, lt_hi[...])
    out_ref[0] = fy[y] + spread

    for i in range(8):
        @pl.when(jnp.logical_not(p0_self(i)))
        def _():
            p0_copy(i).wait_send()

    @pl.when(tm > 0)
    def _():
        next_copy.wait_send()

    for d in range(1, 8):
        g1_send(d).wait_send()
        g2_send(d).wait_send()
        h1_send(d).wait_send()
    for d in range(1, 4):
        fx_send(d).wait_send()
        fy_send(d).wait_send()
    for d in range(1, 16):
        h2_send(d).wait_send()

    @pl.when(home)
    def _():
        def drain(s, carry):
            for d in range(1, 4):
                x_send(s, d).wait_send()
            for zz in range(4):
                partner_send(s, zz).wait_send()
            return carry

        lax.fori_loop(0, FINE, drain, 0)

        def drain_sums(s, carry):
            for zz in range(4):
                @pl.when(jnp.logical_not(p2_local(zz)))
                def _():
                    p2_send(s, zz).wait_send()
            return carry

        lax.fori_loop(0, FINE - 1, drain_sums, 0)

    def drain_products(s, carry):
        for i in range(8):
            @pl.when(jnp.logical_not(p1_local(i)))
            def _():
                p1_send(s, i).wait_send()
        return carry

    lax.fori_loop(0, FINE - 1, drain_products, 0)


def local(starts, operator, coarse_left, coarse_right):
    rows_here, width = operator.shape
    rank = coarse_right.shape[1]
    steps = FINE - 1
    dma = pltpu.SemaphoreType.DMA
    vmem = pltpu.VMEM
    scratch = [
        vmem((E, rows_here), F32),
        vmem((E, rows_here), F32),
        vmem((8, rows_here // 8, width), F32),
        vmem((rows_here, width), BF16),
        vmem((rows_here, width), BF16),
        vmem((rows_here, rank), F32),
        vmem((rows_here, rank), F32),
        vmem((rows_here, rank), BF16),
        vmem((rows_here, rank), BF16),
        vmem((rank, rows_here), BF16),
        vmem((rank, rows_here), BF16),
        vmem((SLICES, E, BLK), F32),
        vmem((FINE, 4, BLK, LANES), F32),
        vmem((width, 2 * LANES), BF16),
        vmem((steps, 8, BLK, LANES), F32),
        vmem((steps, 4, 4, BLK, LANES), F32),
        vmem((steps, 4, BLK, LANES), F32),
        vmem((steps, 4, BLK, LANES), F32),
        vmem((4, 4, E, rows_here), F32),
        vmem((4, 4, E, rows_here), F32),
        vmem((4, E, rows_here), F32),
        vmem((4, E, rows_here), F32),
        vmem((8, rank // 8, rank), F32),
        vmem((8, rank // 8, rank), F32),
        vmem((rank // 8, rank), F32),
        vmem((8, rank // 8, rank), F32),
        vmem((4, rank, rank), F32),
        vmem((E, rank), F32),
        vmem((8, E, rank), F32),
        vmem((E, rank), F32),
        vmem((SLICES + 1, E, rank), F32),
        vmem((SLICES, E, rank), F32),
        dma((11,)),
        dma((2,)),
        dma((8,)), dma((16,)),
        dma((steps, 8)), dma((steps, 4, 4)),
        dma((steps, 4)), dma((steps, 4)),
        dma((FINE, 4)), dma((FINE, 4)), dma((FINE, 4)),
        dma((4,)), dma((4,)), dma((4,)), dma((4,)),
        dma((8,)), dma((8,)), dma((8,)), dma((8,)),
        dma((8,)), dma((8,)), dma((16,)), dma((16,)),
    ]
    return pl.pallas_call(
        kernel,
        out_shape=jax.ShapeDtypeStruct(starts.shape, F32),
        in_specs=[pl.BlockSpec(memory_space=pl.ANY)] * 4,
        out_specs=pl.BlockSpec(memory_space=pltpu.VMEM),
        scratch_shapes=scratch,
        compiler_params=pltpu.CompilerParams(
            collective_id=0, has_side_effects=True, vmem_limit_bytes=63 * 1024 * 1024
        ),
    )(starts, operator, coarse_left, coarse_right)


def solution(mesh):
    in_specs = (P("tm", None, "row"), P("row", "tm"), P("row", None), P("row", None))
    out_specs = P("tm", None, "row")
    return jax.shard_map(local, mesh=mesh, in_specs=in_specs, out_specs=out_specs, check_vma=False)
```
